32 devices in a mesh: row: 4 (over x, core), col: 8 (over z, y).
Axes of the slice: x: 2, y: 2, z: 4, core: 2. Of those that a mesh axis runs over, the one named last changes fastest.
Arguments:
- hamiltonian: bfloat16 [2912, 2912], P('row', 'col'), may hold values from -6 to 6
- new_atom: int32 [224], replicated, may hold values from 0 to 223, as said below
- pattern: int32 [224, 224], P('row', 'col'), may hold values 0 or 1
Outputs:
- sign_matrix: float32 [2912, 2912], P('row', 'col')
The draws below stay inside these ranges and needn't reach their ends.
Inputs may be any that keep to these rules, and one draw needn't show every extreme that they name: `new_atom`: each old atom appears once. Block column b holds atoms b * 28 to (b + 1) * 28 - 1 in both orders. For each new block column d and each v from 0 to 27, exactly one atom of new block column d comes from old block column (d - 1 - (v mod 8)) mod 8, so the number of atoms that old block column b sends to new block column (b + k) mod 8 is the number of such v with (1 + v) mod 8 = k.
All inputs are finite; a program needn't handle non-finite values. No bound on the sum of `pattern` on one device may be relied on, other than what follows from the above.
Results may differ from the reference program's by a relative error of at most 0.0029.
Values may be sent and summed in bfloat16 or wider, within the bound.
A program may use at most 64 MiB of HBM per device.

```python
import jax
import jax.numpy as jnp
from jax import lax

NBF = 13
ATOM_COL = 28
ATOMS = 224
ORDER = 2912
N_COL = 8


def draw_new_atom(key, part):
    slot_key, arrive_key = jax.random.split(jax.random.fold_in(key, 17))
    slot_keys = jax.random.split(slot_key, N_COL)
    arrive_keys = jax.random.split(arrive_key, N_COL)
    slot_inverse = jax.vmap(lambda k: jax.random.permutation(k, ATOM_COL))(slot_keys).astype(jnp.int32)
    arrival = jax.vmap(lambda k: jax.random.permutation(k, ATOM_COL))(arrive_keys).astype(jnp.int32)
    target = jnp.arange(N_COL, dtype=jnp.int32)[:, None]
    source = (target - 1 - arrival % N_COL) % N_COL
    old_atom = source * ATOM_COL + slot_inverse[source, arrival]
    return old_atom.reshape(-1).astype(jnp.int32)


def set_ends(result, key, smallest, top_value):
    dims = result.shape
    spot = [jax.random.randint(jax.random.fold_in(key, axis), (), 0, dims[axis]) for axis in range(len(dims))]
    result = result.at[tuple(spot)].set(smallest)
    longest = dims.index(max(dims))
    spot[longest] = (spot[longest] + 1) % dims[longest]
    return result.at[tuple(spot)].set(top_value)


def block_scale(key, dims, cuts, smallest, largest):
    gain, own = 1.0, jax.random.fold_in(key, 6)
    for dim, blocks in cuts:
        heights = jnp.exp(jax.random.uniform(jax.random.fold_in(own, dim), (blocks,), jnp.float32, smallest / len(cuts), largest / len(cuts)))
        gain = gain * jnp.repeat(heights, dims[dim] // blocks).reshape([-1 if axis == dim else 1 for axis in range(len(dims))])
    return gain


def normal_values(stream_key, dims, deviation, most, shards=(), held_as=jnp.bfloat16):
    result = jax.random.normal(stream_key, dims, jnp.float32) * deviation
    if len(shards) > 0:
        result = block_scale(stream_key, dims, shards, -0.22, 0.18) * result
    return jnp.clip(result, min=-most, max=most).astype(held_as)


def setup_inputs(seed: int = 0) -> dict:
    streams_of = jax.random.split(jax.random.key(seed), 4)
    hamiltonian = normal_values(streams_of[0], (ORDER, ORDER), 1.0, 6.0, ((0, 4), (1, 8)))
    new_atom = draw_new_atom(jax.random.fold_in(streams_of[3], 71), 0)
    pattern = set_ends((jax.random.randint(streams_of[2], (ATOMS, ATOMS), 0, 3) < 1).astype(jnp.int32), jax.random.fold_in(streams_of[2], 1), 0, 1)
    return dict(hamiltonian=hamiltonian, new_atom=new_atom, pattern=pattern)


def reference(hamiltonian, new_atom, pattern):
    order_all = ATOMS * NBF
    index = (new_atom[:, None] * NBF + jnp.arange(NBF, dtype=jnp.int32)[None, :]).reshape(-1).astype(jnp.int32)
    moved = jnp.take(jnp.take(hamiltonian, index, axis=0), index, axis=1)
    keep = jnp.broadcast_to(pattern.astype(jnp.float32)[:, None, :, None], (ATOMS, NBF, ATOMS, NBF)).reshape(order_all, order_all)
    masked = moved.astype(jnp.float32) * keep
    total = jnp.sum(masked * masked)
    start = (masked * lax.rsqrt(total / order_all)).astype(jnp.bfloat16)
    square = (jnp.dot(start, start, preferred_element_type=jnp.float32) * keep).astype(jnp.bfloat16)
    cube = jnp.dot(start, square, preferred_element_type=jnp.float32) * keep
    return keep * (1.5 * start.astype(jnp.float32) - 0.5 * cube)
```

```python
import jax
import jax.numpy as jnp
from jax import lax
from jax.sharding import PartitionSpec as P

NBF = 13
BF = jnp.bfloat16
F32 = jnp.float32


def mm(a, b):
    return jnp.dot(a, b, preferred_element_type=F32)


def spread(n):
    i = lax.broadcasted_iota(jnp.int32, (n * NBF, n), 0)
    a = lax.broadcasted_iota(jnp.int32, (n * NBF, n), 1) * NBF
    return (i >= a) & (i < a + NBF)


def on_device(hamiltonian, new_atom, pattern):
    rows_here, cols_here = hamiltonian.shape
    order = rows_here * lax.axis_size("row")
    atoms = order // NBF
    ar, ac = pattern.shape
    row_here = lax.axis_index("row")
    col_here = lax.axis_index("col")
    panel = lax.all_gather(hamiltonian, "col", axis=1, tiled=True)
    pat = lax.all_gather(pattern.astype(BF), ("row", "col"), axis=0, tiled=False)
    n_row, n_col = lax.axis_size("row"), lax.axis_size("col")
    pat = pat.reshape(n_row, n_col, ar, ac).transpose(0, 2, 1, 3).reshape(atoms, atoms)
    old = jnp.arange(atoms, dtype=jnp.int32)
    perm = (new_atom[:, None] == old[None, :]).astype(BF)
    mine = (new_atom[None, :] == row_here * ar + jnp.arange(ar, dtype=jnp.int32)[:, None]).astype(BF)
    pat_rows = mm(mine, pat).astype(BF)
    e_row = spread(ar)
    e_col = spread(ac)
    e_rowb = e_row.astype(BF)
    rows_masked = mm(e_rowb, mm(pat_rows, perm).astype(BF)).astype(BF)
    keep = mm(rows_masked, spread(atoms).astype(BF).T).astype(BF)
    m = panel * keep
    total = lax.psum(jnp.sum(m.astype(F32) ** 2), "row")
    s = lax.rsqrt(total / order)

    def old_index(n, here, e):
        mine_atoms = lax.dynamic_slice_in_dim(new_atom, here * n, n)
        base = jnp.sum(jnp.where(e, (mine_atoms - jnp.arange(n, dtype=jnp.int32))[None, :], 0), axis=1)
        return base * NBF + jnp.arange(n * NBF, dtype=jnp.int32)

    full = jnp.arange(order, dtype=jnp.int32)
    pick_col = (full[:, None] == old_index(ac, col_here, e_col)[None, :]).astype(BF)
    pick_row = (old_index(ar, row_here, e_row)[:, None] == full[None, :]).astype(BF)
    right = lax.all_gather(mm(m, pick_col).astype(BF), "row", axis=0, tiled=True)
    e_colt = e_col.astype(BF).T
    here_cols = lax.dynamic_slice_in_dim(pat_rows, col_here * ac, ac, axis=1)
    keep_sq = mm(mm(e_rowb, here_cols).astype(BF), e_colt)
    square = (mm(m, right) * (s * s) * keep_sq).astype(BF)
    square = lax.all_gather(square, "row", axis=0, tiled=True)
    cube = lax.all_gather((mm(m, square) * s).astype(BF), "row", axis=0, tiled=True)
    start = (mm(pick_row, right) * s).astype(BF).astype(F32)
    keep_out = mm(mm(e_rowb, pattern.astype(BF)).astype(BF), e_colt)
    return keep_out * (1.5 * start - 0.5 * mm(pick_row, cube))


def solution(mesh):
    in_specs = (P("row", "col"), P(), P("row", "col"))
    out_specs = P("row", "col")
    return jax.shard_map(
        on_device, mesh=mesh, in_specs=in_specs, out_specs=out_specs, check_vma=False
    )
```

```python
import functools

import jax
import jax.numpy as jnp
from jax import lax
from jax.experimental import pallas as pl
from jax.experimental.pallas import tpu as pltpu
from jax.sharding import PartitionSpec as P

NBF = 13
LANE = 128
BF = jnp.bfloat16
F32 = jnp.float32
I32 = jnp.int32
MESH = pl.DeviceIdType.MESH


def up(n, k):
    return -(-n // k) * k


def mm(a, b):
    return jnp.dot(a, b, preferred_element_type=F32)


def mm_nt(a, b):
    return lax.dot_general(a, b, (((1,), (1,)), ((), ())), preferred_element_type=F32)


def spread(rows, lanes, base, count):
    i = lax.broadcasted_iota(I32, (rows, lanes), 0)
    a = lax.broadcasted_iota(I32, (rows, lanes), 1) - base
    hit = (a >= 0) & (a < count) & (i >= a * NBF) & (i < a * NBF + NBF)
    return jnp.where(hit, 1.0, 0.0).astype(BF)


def kernel(
    n_row, n_col, atoms_col, order,
    h_ref, pat_ref, selrow_ref, selcol_ref, poscol_ref, posrow_ref,
    out_ref,
    panel, m, bt, st, ct, acc, pt_in, pt_all, pt_old, tot, tot_all, er,
    own_sem, p1_send, p1_recv, p2_send, p2_recv, t_send, t_recv,
    g_send, g_recv, r_send, r_recv, f_send,
):
    ratio = n_col // n_row
    blk = h_ref.shape[2]
    live = up(atoms_col * NBF, 16)
    av = pat_ref.shape[0]
    outer = n_col // 2
    nx = n_row // 2
    pieces = blk // LANE
    row = lax.axis_index("row")
    col = lax.axis_index("col")
    hi, lo = col // 2, col % 2
    x, core = row // 2, row % 2
    peer_row = x * 2 + 1 - core

    def chunk_piece(c, t):
        return panel.at[c, t, pl.ds(0, live), :]

    own = []
    for t in range(ratio):
        cp = pltpu.make_async_copy(h_ref.at[t, pl.ds(0, live), :], chunk_piece(col, t), own_sem.at[t])
        cp.start()
        own.append(cp)

    barrier = pltpu.get_barrier_semaphore()
    for k in range(1, n_row):
        pl.semaphore_signal(barrier, inc=1, device_id={"row": (row + k) % n_row, "col": col}, device_id_type=MESH)
    for k in range(1, n_col):
        pl.semaphore_signal(barrier, inc=1, device_id={"row": row, "col": (col + k) % n_col}, device_id_type=MESH)
    pl.semaphore_wait(barrier, n_row + n_col - 2)

    def hop(c, t, way):
        to = [col + 2, col - 2, hi * 2 + 1 - lo][way]
        return pltpu.make_async_remote_copy(
            src_ref=chunk_piece(c, t), dst_ref=chunk_piece(c, t),
            send_sem=g_send.at[way, c, t], recv_sem=g_recv.at[c, t],
            device_id={"row": row, "col": to}, device_id_type=MESH,
        )

    for t in range(ratio):
        own[t].wait()

        @pl.when(hi + 1 < outer)
        def _():
            hop(col, t, 0).start()

        @pl.when(hi > 0)
        def _():
            hop(col, t, 1).start()

        hop(col, t, 2).start()

    def p1(k):
        return pltpu.make_async_remote_copy(
            src_ref=pat_ref, dst_ref=pt_in.at[row], send_sem=p1_send.at[k], recv_sem=p1_recv.at[row],
            device_id={"row": (row + k) % n_row, "col": col}, device_id_type=MESH,
        )

    def p2(k):
        return pltpu.make_async_remote_copy(
            src_ref=pt_all.at[col], dst_ref=pt_all.at[col], send_sem=p2_send.at[k], recv_sem=p2_recv.at[col],
            device_id={"row": row, "col": (col + k) % n_col}, device_id_type=MESH,
        )

    for k in range(1, n_row):
        p1(k).start()
    panel[:, :, live:, :] = jnp.zeros((n_col, ratio, blk - live, blk), BF)
    for t in range(ratio):
        er[t * blk : (t + 1) * blk, :] = spread(blk, LANE, t * atoms_col, atoms_col)
    ec = spread(blk, av, 0, atoms_col)
    pt_in[row] = pat_ref[...]
    acc[...] = jnp.zeros_like(acc)
    tot[...] = jnp.zeros_like(tot)
    for k in range(1, n_row):
        src = (row + k) % n_row
        pltpu.make_async_copy(pt_in.at[src], pt_in.at[src], p1_recv.at[src]).wait()
    old_rows = jnp.zeros((av, LANE), F32)
    for r in range(n_row):
        old_rows += mm(pt_in[r], selrow_ref[r])
    pt_all[col] = old_rows.astype(BF)
    for k in range(1, n_col):
        p2(k).start()
    for k in range(1, n_col):
        src = (col + k) % n_col
        pltpu.make_async_copy(pt_all.at[src], pt_all.at[src], p2_recv.at[src]).wait()
    everything = pt_all[...].reshape(n_col * av, LANE)
    for c in range(n_col):
        pt_old[c] = mm(selcol_ref[c], everything).astype(BF)

    def arrived(c, t):
        pltpu.make_async_copy(chunk_piece(c, t), chunk_piece(c, t), g_recv.at[c, t]).wait()

    def process(c):
        mask_rows = mm_nt(er[...], pt_old[c]).astype(BF)
        keep = mm_nt(mask_rows, ec)
        j = lax.broadcasted_iota(I32, (blk, blk), 1)
        pick = jnp.where(poscol_ref[...] == j + c * blk, 1.0, 0.0).astype(BF)
        for t in range(ratio):
            part = jnp.where(keep[t * blk : (t + 1) * blk] > 0.5, panel[c, t].astype(F32), 0.0)
            tot[...] += jnp.sum((part * part).reshape(blk // 8, 8, blk), axis=0)
            part = part.astype(BF)
            m[c, t * blk : (t + 1) * blk, :] = part
            acc[:, t * blk : (t + 1) * blk] += mm_nt(pick, part)

    def step(d, _):
        for way in range(2):
            src = hi - d if way == 0 else hi + d
            ok = (d > 0) & (d < outer) & (src >= 0) & (src < outer)

            @pl.when(ok)
            def _():
                c = src * 2 + lo
                more = hi + 1 < outer if way == 0 else hi > 0
                for t in range(ratio):
                    arrived(c, t)

                    @pl.when(more)
                    def _():
                        hop(c, t, way).start()

                    hop(c, t, 2).start()

        def candidate(k, _):
            kind, way = k // 2, k % 2
            dist = d - kind
            src = hi + (1 - 2 * way) * dist
            ok = (dist >= 0) & (dist < outer) & (src >= 0) & (src < outer) & ((dist > 0) | (way == 0))

            @pl.when(ok)
            def _():
                c = src * 2 + jnp.where(kind == 0, lo, 1 - lo)

                @pl.when(kind == 1)
                def _():
                    for t in range(ratio):
                        arrived(c, t)

                process(c)

            return 0

        lax.fori_loop(0, 4, candidate, 0)
        return 0

    lax.fori_loop(0, outer + 1, step, 0)

    def share(buf, stage, p):
        def part(r):
            return buf.at[r, pl.ds(p * LANE, LANE), :]

        def send(r, to, sem):
            return pltpu.make_async_remote_copy(
                src_ref=part(r), dst_ref=part(r), send_sem=sem, recv_sem=r_recv.at[stage, p, r],
                device_id={"row": to, "col": col}, device_id_type=MESH,
            )

        return (
            [send(row, (x + k) % nx * 2 + core, r_send.at[stage, p, k]) for k in range(1, nx)]
            + [send(row, peer_row, r_send.at[stage, p, 0])],
            [send((x + k) % nx * 2 + core, peer_row, f_send.at[stage, p, k]) for k in range(1, nx)],
        )

    def start_own(buf, stage, p):
        for cp in share(buf, stage, p)[0]:
            cp.start()

    def got(buf, stage, p, r):
        ref = buf.at[r, pl.ds(p * LANE, LANE), :]
        pltpu.make_async_copy(ref, ref, r_recv.at[stage, p, r]).wait()

    def relay(buf, stage, p):
        onward = share(buf, stage, p)[1]
        for k in range(1, nx):
            got(buf, stage, p, (x + k) % nx * 2 + core)
            onward[k - 1].start()

    def finish(buf, stage, p):
        for k in range(nx):
            got(buf, stage, p, (x + k) % nx * 2 + 1 - core)

    def drain(buf, stage, p):
        first, onward = share(buf, stage, p)
        for cp in first + onward:
            cp.wait_send()

    def t_copy(k):
        return pltpu.make_async_remote_copy(
            src_ref=tot_all.at[row], dst_ref=tot_all.at[row], send_sem=t_send.at[k], recv_sem=t_recv.at[row],
            device_id={"row": (row + k) % n_row, "col": col}, device_id_type=MESH,
        )

    part_sum = tot[:, 0:LANE]
    for q in range(1, pieces):
        part_sum += tot[:, q * LANE : (q + 1) * LANE]
    tot_all[row] = part_sum
    for p in range(pieces):
        bt[row, p * LANE : (p + 1) * LANE, :] = acc[p * LANE : (p + 1) * LANE, :].astype(BF)
        start_own(bt, 0, p)
    for k in range(1, n_row):
        t_copy(k).start()
    for k in range(1, n_row):
        src = (row + k) % n_row
        pltpu.make_async_copy(tot_all.at[src], tot_all.at[src], t_recv.at[src]).wait()
    total = jnp.sum(jnp.sum(tot_all[...], axis=0), axis=(0, 1), keepdims=True)
    s = lax.rsqrt(total / order)

    def panel_product(buf, p):
        result = jnp.zeros((LANE, ratio * blk), F32)
        for c in range(n_col):
            t = c % ratio
            result += mm_nt(buf[c // ratio, p * LANE : (p + 1) * LANE, t * blk : (t + 1) * blk], m[c])
        return result

    mask_cols = mm(ec, pt_all[col]).astype(BF)
    for p in range(pieces):
        relay(bt, 0, p)
    for p in range(pieces):
        finish(bt, 0, p)
        keep = mm_nt(mask_cols[p * LANE : (p + 1) * LANE], er[...])
        square = panel_product(bt, p) * (s * s)
        st[row, p * LANE : (p + 1) * LANE, :] = jnp.where(keep > 0.5, square, 0.0).astype(BF)
        start_own(st, 1, p)

    def pick_rows(r):
        j = lax.broadcasted_iota(I32, (ratio * blk, ratio * blk), 1)
        return jnp.where(posrow_ref[...] == j + r * (ratio * blk), 1.0, 0.0).astype(BF)

    start = jnp.zeros((ratio * blk, blk), F32)
    for r in range(n_row):
        start += mm_nt(pick_rows(r), bt[r])
    start = 1.5 * (start * s).astype(BF).astype(F32)
    for t in range(ratio):
        out_ref[t] = start[t * blk : (t + 1) * blk]
    for p in range(pieces):
        relay(st, 1, p)
        finish(st, 1, p)
        cube = panel_product(st, p) * s
        ct[row, p * LANE : (p + 1) * LANE, :] = cube.astype(BF)
        start_own(ct, 2, p)
    for p in range(pieces):
        relay(ct, 2, p)
    for p in range(pieces):
        finish(ct, 2, p)
    mine = mm_nt(er[...], pat_ref[...]).astype(BF)
    keep = mm_nt(mine, ec)
    cube = jnp.zeros((ratio * blk, blk), F32)
    for r in range(n_row):
        cube += mm_nt(pick_rows(r), ct[r])
    for t in range(ratio):
        part = slice(t * blk, (t + 1) * blk)
        out_ref[t] = jnp.where(keep[part] > 0.5, out_ref[t] - 0.5 * cube[part], 0.0)

    for k in range(1, n_row):
        p1(k).wait_send()
        t_copy(k).wait_send()
    for k in range(1, n_col):
        p2(k).wait_send()

    def sent(q, _):
        c = q * 2 + lo
        for t in range(ratio):

            @pl.when((q <= hi) & (hi + 1 < outer))
            def _():
                hop(c, t, 0).wait_send()

            @pl.when((q >= hi) & (hi > 0))
            def _():
                hop(c, t, 1).wait_send()

            hop(c, t, 2).wait_send()
        return 0

    lax.fori_loop(0, outer, sent, 0)
    for stage, buf in enumerate((bt, st, ct)):
        for p in range(pieces):
            drain(buf, stage, p)


def on_device(hamiltonian, new_atom, pattern):
    rows_here, cols_here = hamiltonian.shape
    n_row, n_col = lax.axis_size("row"), lax.axis_size("col")
    ratio = n_col // n_row
    ar, ac = pattern.shape
    order = rows_here * n_row
    blk = up(cols_here, LANE)
    av = up(ac, 16)
    row_here = lax.axis_index("row")
    col_here = lax.axis_index("col")
    pad = blk - cols_here
    h = jnp.pad(hamiltonian.reshape(ratio, cols_here, cols_here), ((0, 0), (0, pad), (0, pad)))
    pat_t = jnp.pad(pattern.astype(BF).T, ((0, av - ac), (0, LANE - ar)))
    by_row = jnp.pad(new_atom.reshape(n_row, ar), ((0, 0), (0, LANE - ar)), constant_values=-1)
    i = jnp.arange(LANE, dtype=I32)
    selrow = ((by_row[:, :, None] == row_here * ar + i) & (i < ar)).astype(BF)
    by_col = jnp.pad(new_atom.reshape(n_col, ac), ((0, 0), (0, av - ac)), constant_values=-1).reshape(-1)
    v = jnp.arange(av, dtype=I32)
    old = jnp.arange(n_col, dtype=I32)[:, None] * ac + v[None, :]
    selcol = ((by_col[None, None, :] == old[:, :, None]) & (v < ac)[None, :, None]).astype(BF)
    place = new_atom // ac * blk + new_atom % ac * NBF

    def positions(here):
        mine = lax.dynamic_slice_in_dim(place, here * ac, ac)
        q = jnp.arange(blk, dtype=I32)
        a = jnp.arange(ac, dtype=I32)
        hit = (q[:, None] >= a * NBF) & (q[:, None] < a * NBF + NBF)
        base = jnp.sum(jnp.where(hit, (mine - a * NBF)[None, :], 0), axis=1)
        return jnp.where(q < ac * NBF, base + q, -1)

    poscol = positions(col_here)[:, None]
    posrow = jnp.concatenate([positions(row_here * ratio + t) for t in range(ratio)])[:, None]
    pieces = blk // LANE
    vm = pl.BlockSpec(memory_space=pltpu.VMEM)
    dma = pltpu.SemaphoreType.DMA
    wide = ratio * blk
    out = pl.pallas_call(
        functools.partial(kernel, n_row, n_col, ac, float(order)),
        out_shape=jax.ShapeDtypeStruct((ratio, blk, blk), F32),
        in_specs=[pl.BlockSpec(memory_space=pl.ANY)] + [vm] * 5,
        out_specs=vm,
        scratch_shapes=[
            pltpu.VMEM((n_col, ratio, blk, blk), BF),
            pltpu.VMEM((n_col, wide, blk), BF),
            pltpu.VMEM((n_row, blk, wide), BF),
            pltpu.VMEM((n_row, blk, wide), BF),
            pltpu.VMEM((n_row, blk, wide), BF),
            pltpu.VMEM((blk, wide), F32),
            pltpu.VMEM((n_row, av, LANE), BF),
            pltpu.VMEM((n_col, av, LANE), BF),
            pltpu.VMEM((n_col, av, LANE), BF),
            pltpu.VMEM((8, blk), F32),
            pltpu.VMEM((n_row, 8, LANE), F32),
            pltpu.VMEM((wide, LANE), BF),
            dma((ratio,)),
            dma((n_row,)),
            dma((n_row,)),
            dma((n_col,)),
            dma((n_col,)),
            dma((n_row,)),
            dma((n_row,)),
            dma((3, n_col, ratio)),
            dma((n_col, ratio)),
            dma((3, pieces, n_row)),
            dma((3, pieces, n_row)),
            dma((3, pieces, n_row)),
        ],
        compiler_params=pltpu.CompilerParams(
            collective_id=0, has_side_effects=True, vmem_limit_bytes=60 * 1024 * 1024
        ),
    )(h, pat_t, selrow, selcol, poscol, posrow)
    return out[:, :cols_here, :cols_here].reshape(rows_here, cols_here)


def solution(mesh):
    in_specs = (P("row", "col"), P(), P("row", "col"))
    out_specs = P("row", "col")
    return jax.shard_map(
        on_device, mesh=mesh, in_specs=in_specs, out_specs=out_specs, check_vma=False
    )
```
